32 devices in a mesh: wave: 8 (over z, y), lev: 4 (over x, core).
Axes of the slice: x: 2, y: 2, z: 4, core: 2. Of those that a mesh axis runs over, the one named last changes fastest.
Arguments:
- spectral: bfloat16 [32, 6, 64, 1280], P('wave', None, 'lev'), may hold values from -0.01171875 to 0.01171875
- legendre: bfloat16 [32, 640, 1280], P('wave'), may hold values from -4 to 4
- wave_ids: int32 [32], replicated, may hold values from 0 to 1279, as said below
- trunc_lengths: int32 [32], replicated, may hold values from 1 to 1280, as said below
- cycle_points: int32 [1280], replicated, may hold values from 20 to 2560, as said below
- grid_coef: float32 [1280, 2560], P('wave'), may hold values from -6 to 6
- cycle_weights: float32 [640], replicated, may hold values from 0.1 to 2
- modes_in: bfloat16 [64, 64], replicated, may hold values from -0.75 to 0.75
- modes_out: bfloat16 [64, 64], replicated, may hold values from -0.75 to 0.75
- depths: float32 [64], replicated, may hold values from 0.05 to 20
Outputs:
- update: bfloat16 [32, 6, 64, 1280], P('wave', None, 'lev')
The draws below stay inside these ranges and needn't reach their ends.
Inputs may be any that keep to these rules, and one draw needn't show every extreme that they name: `wave_ids`: distinct zonal wavenumbers; one slot holds wavenumber 0. `trunc_lengths`: the length of slot m is at most 1280 minus wave_ids[m] and at least half of that; the slot of wavenumber 0 has length 1280. `cycle_points`: multiples of 4; cycle j and cycle 1280 - 1-j have the same count; cycles near the equator have 2560.
All inputs are finite; a program needn't handle non-finite values.
Results may differ from the reference program's by a relative error of at most 0.011.
Values may be sent and summed in bfloat16 or wider, within the bound.
No kernel may reach another device: no remote copies, remote signals or barrier semaphores. Data moves between devices by JAX's collectives and lax.ppermute only.
A program may use at most 128 MiB of HBM per device.

```python
import math
import jax
import jax.numpy as jnp
from jax import lax

NT = 1280
NLAT = 1280
NHALF = 640
LONMAX = 2560
FIELDS = 3
M_WIN = 32
LEVELS = 64


def wave_table(key):
    base_key = jax.random.fold_in(key, 11)
    others = jax.random.permutation(jax.random.fold_in(base_key, 1), NT - 1)[:M_WIN - 1] + 1
    chosen = jnp.concatenate([jnp.zeros((1,), jnp.int32), others.astype(jnp.int32)])
    shuffle = jax.random.permutation(jax.random.fold_in(base_key, 2), M_WIN)
    waves = chosen[shuffle]
    jitter = jax.random.randint(jax.random.fold_in(base_key, 3), (M_WIN,), 0, 4)
    jitter = jnp.where(waves == 0, 0, jitter)
    headroom = NT - waves
    shorten = jnp.minimum(8 * jitter, headroom // 2)
    return (waves.astype(jnp.int32), (headroom - shorten).astype(jnp.int32))


def draw_wave_ids(key, part):
    return wave_table(key)[0]


def draw_trunc_lengths(key, part):
    return wave_table(key)[1]


def draw_cycle_points(key, part):
    cycle_index = jnp.arange(NHALF, dtype=jnp.int32)
    jitter = jax.random.randint(jax.random.fold_in(key, 21), (NHALF,), 0, 4)
    northern = jnp.minimum(LONMAX, 20 + 4 * cycle_index + 4 * jitter)
    return jnp.concatenate([northern, northern[::-1]]).astype(jnp.int32)


def levels(key, extent, shards, least, high):
    def one(dim, blocks):
        heights = jax.random.uniform(jax.random.fold_in(jax.random.fold_in(key, 6), dim), (blocks,), jnp.float32, least / len(shards), high / len(shards))
        return jnp.repeat(jnp.exp(heights), extent[dim] // blocks).reshape((-1,) + (1,) * (len(extent) - dim - 1))

    gain = one(*shards[0])
    for cut in shards[1:]:
        gain = gain * one(*cut)
    return gain


def noise(stream_key, dims, width, bound, split=(), kind=jnp.bfloat16):
    values = width * jax.random.normal(stream_key, dims, jnp.float32)
    if split:
        values = values * levels(stream_key, dims, split, -0.22, 0.18)
    return jnp.clip(values, -bound, bound).astype(kind)


def setup_inputs(seed: int = 0) -> dict:
    keys = jax.random.split(jax.random.key(seed), 11)
    spectral = noise(keys[0], (M_WIN, 2 * FIELDS, LEVELS, NT), 0.002, 0.01171875, ((0, 8), (2, 4)))
    legendre = noise(keys[1], (M_WIN, NHALF, NT), 1.0, 4.0, ((0, 8),))
    wave_ids = draw_wave_ids(jax.random.fold_in(keys[10], 71), 0)
    trunc_lengths = draw_trunc_lengths(jax.random.fold_in(keys[10], 71), 0)
    cycle_points = draw_cycle_points(jax.random.fold_in(keys[10], 71), 0)
    grid_coef = noise(keys[5], (NLAT, LONMAX), 1.0, 6.0, ((0, 8),), jnp.float32)
    cycle_weights = jnp.clip(jnp.exp(jax.random.uniform(keys[6], (NHALF,), jnp.float32, math.log(0.1), math.log(2.0))), 0.1, 2.0)
    modes_in = noise(keys[7], (LEVELS, LEVELS), LEVELS ** -0.5, 0.75)
    modes_out = noise(keys[8], (LEVELS, LEVELS), LEVELS ** -0.5, 0.75)
    depths = jnp.clip(jnp.exp(jax.random.uniform(keys[9], (LEVELS,), jnp.float32, math.log(0.05), math.log(20.0))), 0.05, 20.0)
    return {"spectral": spectral, "legendre": legendre, "wave_ids": wave_ids, "trunc_lengths": trunc_lengths, "cycle_points": cycle_points, "grid_coef": grid_coef, "cycle_weights": cycle_weights, "modes_in": modes_in, "modes_out": modes_out, "depths": depths}


def trig_rows(wave_ids, cycle_count, lon_max):
    longitude = jnp.arange(lon_max, dtype=jnp.int32)
    counts = cycle_count[:, None, None]
    phase_idx = (wave_ids[None, :, None] * longitude[None, None, :]) % counts
    angles = (2.0 * jnp.pi) * phase_idx.astype(jnp.float32) / counts.astype(jnp.float32)
    live_mask = (longitude[None, None, :] < counts) & (2 * wave_ids[None, :, None] < counts)
    cosine = jnp.where(live_mask, jnp.cos(angles), 0.0)
    sine_part = jnp.where(live_mask, -jnp.sin(angles), 0.0)
    return jnp.stack([cosine, sine_part], axis=1).astype(jnp.bfloat16)


def cycle_trip(fourier, wave_ids, cycle_count, coef_rows):
    wave_total, channels, items, group_size = fourier.shape
    fields = channels // 2
    polys = trig_rows(wave_ids, cycle_count, coef_rows.shape[1])
    factor = jnp.where(wave_ids == 0, 1.0, 2.0).astype(jnp.bfloat16)
    weighted = (fourier * factor[:, None, None, None]).reshape(wave_total, 2, fields, items, group_size)
    grid_vals = jnp.einsum("mrfig,grmk->gfik", weighted.astype(jnp.float32), polys.astype(jnp.float32))
    tendency = (grid_vals * (coef_rows[:, None, None, :] + jnp.roll(grid_vals, -1, axis=1))).astype(jnp.bfloat16)
    analysed = jnp.einsum("gfik,grmk->mrfig", tendency.astype(jnp.float32), polys.astype(jnp.float32))
    analysed = analysed / cycle_count.astype(jnp.float32)
    return analysed.astype(jnp.bfloat16).reshape(wave_total, channels, items, group_size)


def reference(spectral, legendre, wave_ids, trunc_lengths, cycle_points, grid_coef, cycle_weights, modes_in, modes_out, depths):
    wave_total, channels, levels_total, spec_len = spectral.shape
    half_lat = legendre.shape[1]
    lat_total = 2 * half_lat
    position = jnp.arange(spec_len, dtype=jnp.int32)
    parity_sign = jnp.where(position % 2 == 0, 1.0, -1.0).astype(jnp.bfloat16)

    def inverse_one(packed):
        coeffs, polys, length = packed
        flat = coeffs.reshape(-1, spec_len)
        flat = jnp.where(position[None, :] < length, flat, jnp.zeros_like(flat))
        northern = jnp.dot(flat, polys.T, preferred_element_type=jnp.float32)
        southern = jnp.dot(flat * parity_sign[None, :], polys.T, preferred_element_type=jnp.float32)
        joined = jnp.concatenate([northern, jnp.flip(southern, axis=1)], axis=1).astype(jnp.bfloat16)
        return joined.reshape(channels, levels_total, lat_total)

    fourier = lax.map(inverse_one, (spectral, legendre, trunc_lengths))

    group_size = math.gcd(lat_total, 32)
    groups = lat_total // group_size
    stacked = jnp.moveaxis(fourier.reshape(wave_total, channels, levels_total, groups, group_size), 3, 0)
    counts = cycle_points.reshape(groups, group_size)
    coefs = grid_coef.reshape(groups, group_size, -1)

    def group_trip(packed):
        return cycle_trip(packed[0], wave_ids, packed[1], packed[2])

    results = lax.map(group_trip, (stacked, counts, coefs))
    returned = jnp.moveaxis(results, 0, 3).reshape(wave_total, channels, levels_total, lat_total)

    def forward_one(packed):
        values, polys, length, wavenum = packed
        northern = values[..., :half_lat].astype(jnp.float32)
        southern = jnp.flip(values[..., half_lat:], axis=2).astype(jnp.float32)
        even_part = (cycle_weights * (northern + southern)).astype(jnp.bfloat16).reshape(-1, half_lat)
        odd_part = (cycle_weights * (northern - southern)).astype(jnp.bfloat16).reshape(-1, half_lat)
        from_even = jnp.dot(even_part, polys, preferred_element_type=jnp.float32)
        from_odd = jnp.dot(odd_part, polys, preferred_element_type=jnp.float32)
        coeffs = jnp.where(position[None, :] % 2 == 0, from_even, from_odd)
        coeffs = jnp.where(position[None, :] < length, coeffs, 0.0).astype(jnp.bfloat16)
        coeffs = coeffs.reshape(channels, levels_total, spec_len)
        mode_vals = jnp.einsum("kl,cli->cki", modes_in.astype(jnp.float32), coeffs.astype(jnp.float32))
        degree = (wavenum + position).astype(jnp.float32)
        damp = 1.0 / (1.0 + depths[:, None] * degree[None, :] * (degree[None, :] + 1.0) / float(NT * NT))
        scaled = (mode_vals * damp[None, :, :]).astype(jnp.bfloat16)
        mixed = jnp.einsum("lk,cki->cli", modes_out.astype(jnp.float32), scaled.astype(jnp.float32))
        return mixed.astype(jnp.bfloat16)

    return lax.map(forward_one, (returned, legendre, trunc_lengths, wave_ids))
```

```python
import jax
import jax.numpy as jnp
from jax import lax
from jax.experimental import pallas as pl
from jax.experimental.pallas import tpu as pltpu
from jax.sharding import PartitionSpec as P

LANES = 128
GROUP = 8
UNROLL = 2
CHUNK = 512


def unit_circle(turns):
    half = jnp.floor(2.0 * turns + 0.5)
    angle = (turns - 0.5 * half) * (2.0 * jnp.pi)
    sign = jnp.where(half == 1.0, -1.0, 1.0)
    sq = angle * angle
    cosine = -1.0 / 3628800.0
    for term in (1.0 / 40320.0, -1.0 / 720.0, 1.0 / 24.0, -0.5, 1.0):
        cosine = cosine * sq + term
    sine = -1.0 / 39916800.0
    for term in (1.0 / 362880.0, -1.0 / 5040.0, 1.0 / 120.0, -1.0 / 6.0, 1.0):
        sine = sine * sq + term
    return cosine * sign, sine * angle * sign


def grid_kernel(pts_ref, inv_ref, flip_ref, wave_ref, coef_ref, weights_ref, out_ref, table, tend):
    waves = wave_ref.shape[0]
    points = coef_ref.shape[1]
    rows = weights_ref.shape[2]
    items = rows // 3
    block = pl.program_id(0)
    wave = wave_ref[...]
    lane = lax.broadcasted_iota(jnp.int32, (1, LANES), 1)
    lane_f = lane.astype(jnp.float32)

    def one(pos, slot):
        pts = pts_ref[block * GROUP + pos]
        pts_f = pts.astype(jnp.float32)
        inv = inv_ref[block * GROUP + pos]
        prod = wave * lane_f
        left = prod - jnp.floor(prod * inv) * pts_f
        cosine, sine = unit_circle(left * inv)
        live = jnp.where(2.0 * wave < pts_f, 1.0, 0.0)
        mid_c = cosine[:, LANES // 2:LANES // 2 + 1]
        mid_s = sine[:, LANES // 2:LANES // 2 + 1]
        step_c = jnp.broadcast_to(1.0 - 2.0 * mid_s * mid_s, (waves, LANES))
        step_s = jnp.broadcast_to(2.0 * mid_s * mid_c, (waves, LANES))
        cosine = cosine * live
        sine = -sine * live
        for hi in range(points // LANES):
            table[slot, 0:waves, hi * LANES:(hi + 1) * LANES] = cosine.astype(jnp.bfloat16)
            table[slot, waves:2 * waves, hi * LANES:(hi + 1) * LANES] = sine.astype(jnp.bfloat16)
            cosine, sine = (
                cosine * step_c + sine * step_s,
                sine * step_c - cosine * step_s,
            )
        row = jnp.where(flip_ref[0] == 1, GROUP - 1 - pos, pos)
        weights = weights_ref[pos]
        for start in range(0, points, CHUNK):
            cols = slice(start, start + CHUNK)
            grid = lax.dot_general(
                weights, table[slot, :, cols], (((0,), (0,)), ((), ())),
                preferred_element_type=jnp.float32,
            )
            coef = coef_ref[pl.ds(row, 1), cols]
            rolled = jnp.concatenate([grid[items:], grid[:items]], axis=0)
            col_id = start + lax.broadcasted_iota(jnp.int32, (1, CHUNK), 1)
            value = jnp.where(col_id < pts, grid * (coef + rolled), 0.0)
            tend[slot, :, cols] = value.astype(jnp.bfloat16)
        back = lax.dot_general(
            table[slot], tend[slot], (((1,), (1,)), ((), ())),
            preferred_element_type=jnp.float32,
        )
        out_ref[pos] = (back * inv).astype(jnp.bfloat16)

    def step(index, carry):
        for slot in range(UNROLL):
            one(index * UNROLL + slot, slot)
        return carry

    lax.fori_loop(0, GROUP // UNROLL, step, 0)


def grid_trip(weights, wave_ids, counts, flip, coefs):
    band, modes, rows = weights.shape
    waves = wave_ids.shape[0]
    points = coefs.shape[1]
    blocks = band // GROUP
    wave_f = jnp.broadcast_to(wave_ids.astype(jnp.float32)[:, None], (waves, LANES))
    spec = pltpu.PrefetchScalarGridSpec(
        num_scalar_prefetch=3,
        grid=(blocks,),
        in_specs=[
            pl.BlockSpec((waves, LANES), lambda b, p, v, f: (0, 0)),
            pl.BlockSpec(
                (GROUP, points), lambda b, p, v, f: (jnp.where(f[0] == 1, blocks - 1 - b, b), 0)
            ),
            pl.BlockSpec((GROUP, modes, rows), lambda b, p, v, f: (b, 0, 0)),
        ],
        out_specs=pl.BlockSpec((GROUP, modes, rows), lambda b, p, v, f: (b, 0, 0)),
        scratch_shapes=[
            pltpu.VMEM((UNROLL, modes, points), jnp.bfloat16),
            pltpu.VMEM((UNROLL, rows, points), jnp.bfloat16),
        ],
    )
    return pl.pallas_call(
        grid_kernel,
        grid_spec=spec,
        out_shape=jax.ShapeDtypeStruct((band, modes, rows), jnp.bfloat16),
        compiler_params=pltpu.CompilerParams(dimension_semantics=("arbitrary",)),
    )(counts, 1.0 / counts.astype(jnp.float32), flip, wave_f, coefs, weights)


def on_device(
    spectral,
    legendre,
    wave_ids,
    trunc_lengths,
    cycle_points,
    grid_coef,
    cycle_weights,
    modes_in,
    modes_out,
    depths,
):
    wave_size = lax.axis_size("wave")
    lev_size = lax.axis_size("lev")
    wave_rank = lax.axis_index("wave")
    lev_rank = lax.axis_index("lev")
    wave_local, channels, lev_local, spec_len = spectral.shape
    half_lat = legendre.shape[1]
    wave_total = wave_ids.shape[0]
    fields = channels // 2
    levels = lev_local * lev_size
    items = channels * lev_local
    band = 2 * half_lat // wave_size
    north_bands = wave_size // 2
    own_waves = lax.dynamic_slice_in_dim(wave_ids, wave_rank * wave_local, wave_local)
    own_lengths = lax.dynamic_slice_in_dim(trunc_lengths, wave_rank * wave_local, wave_local)
    position = jnp.arange(spec_len, dtype=jnp.int32)

    factor = jnp.where(own_waves == 0, 1.0, 2.0).astype(jnp.bfloat16)
    live = (position[None, :] < own_lengths[:, None])[:, None, :]
    flat = spectral.reshape(wave_local, items, spec_len) * factor[:, None, None]
    zero = jnp.zeros_like(flat)
    even_in = jnp.where(live & (position % 2 == 0), flat, zero)
    odd_in = jnp.where(live & (position % 2 == 1), flat, zero)
    both = jnp.concatenate([even_in, odd_in], axis=1)
    sums = jnp.einsum("mji,mri->mjr", legendre, both, preferred_element_type=jnp.float32)
    even_sum, odd_sum = sums[..., :items], sums[..., items:]
    north = (even_sum + odd_sum).astype(jnp.bfloat16)
    south = (even_sum - odd_sum).astype(jnp.bfloat16)

    def banded(part):
        return jnp.swapaxes(part, 0, 1).reshape(north_bands, band, wave_local * items)

    blocks = jnp.concatenate([banded(north), banded(south)[::-1]], axis=0)
    got = lax.all_to_all(blocks, "wave", split_axis=0, concat_axis=0, tiled=True)
    weights = got.reshape(wave_size, band, wave_local, 2, fields * lev_local)
    weights = weights.transpose(1, 3, 0, 2, 4).reshape(band, 2 * wave_total, fields * lev_local)

    flip = wave_rank >= north_bands
    north_rank = jnp.where(flip, wave_size - 1 - wave_rank, wave_rank)
    counts = lax.dynamic_slice_in_dim(cycle_points, north_rank * band, band)
    analysed = grid_trip(weights, wave_ids, counts, flip.astype(jnp.int32)[None], grid_coef)

    share = wave_local * channels // lev_size
    per_wave = channels // share
    sent = analysed.reshape(band, 2, wave_total, fields, lev_local)
    sent = sent.transpose(2, 1, 3, 0, 4)
    sent = sent.reshape(wave_size * lev_size, share, band, lev_local)
    back = lax.all_to_all(sent, ("wave", "lev"), split_axis=0, concat_axis=0, tiled=True)
    back = back.reshape(2, north_bands, lev_size, share, band, lev_local)
    northern = back[0].astype(jnp.float32)
    southern = back[1][::-1].astype(jnp.float32)
    scale = cycle_weights.reshape(north_bands, 1, 1, band, 1)
    even = (scale * (northern + southern)).astype(jnp.bfloat16)
    odd = (scale * (northern - southern)).astype(jnp.bfloat16)
    parts = jnp.stack([even, odd])
    parts = parts.transpose(0, 3, 2, 5, 1, 4).reshape(2, share * levels, half_lat)
    column = lev_rank // per_wave
    own_polys = lax.dynamic_index_in_dim(legendre, column, 0, keepdims=False)
    own_wave = lax.dynamic_index_in_dim(own_waves, column, 0, keepdims=False)
    own_length = lax.dynamic_index_in_dim(own_lengths, column, 0, keepdims=False)
    both_out = jnp.einsum("erj,ji->eri", parts, own_polys, preferred_element_type=jnp.float32)
    projected = jnp.where(position % 2 == 0, both_out[0], both_out[1])
    projected = jnp.where(position < own_length, projected, 0.0).astype(jnp.bfloat16)
    projected = projected.reshape(share, levels, spec_len)
    mode_vals = jnp.einsum("ql,cli->cqi", modes_in, projected, preferred_element_type=jnp.float32)
    degree = (own_wave + position).astype(jnp.float32)
    damp = 1.0 / (1.0 + depths[:, None] * degree * (degree + 1.0) / float(spec_len * spec_len))
    scaled = (mode_vals * damp).astype(jnp.bfloat16)
    update = jnp.einsum(
        "lq,cqi->cli", modes_out, scaled, preferred_element_type=jnp.float32
    ).astype(jnp.bfloat16)
    update = lax.all_to_all(update, "lev", split_axis=1, concat_axis=0, tiled=True)
    return update.reshape(wave_local, channels, lev_local, spec_len)


def solution(mesh):
    placed = (
        P("wave", None, "lev", None),
        P("wave", None, None),
        P(),
        P(),
        P(),
        P("wave", None),
        P(),
        P(),
        P(),
        P(),
    )
    return jax.shard_map(
        on_device,
        mesh=mesh,
        in_specs=placed,
        out_specs=P("wave", None, "lev", None),
        check_vma=False,
    )
```

```python
import functools

import jax
import jax.numpy as jnp
from jax import lax
from jax.experimental import pallas as pl
from jax.experimental.pallas import tpu as pltpu
from jax.sharding import PartitionSpec as P

LANES = 128
UNROLL = 2
CHUNK = 512


def unit_circle(turns):
    half = jnp.floor(2.0 * turns + 0.5)
    angle = (turns - 0.5 * half) * (2.0 * jnp.pi)
    sign = jnp.where(half == 1.0, -1.0, 1.0)
    sq = angle * angle
    cosine = -1.0 / 3628800.0
    for term in (1.0 / 40320.0, -1.0 / 720.0, 1.0 / 24.0, -0.5, 1.0):
        cosine = cosine * sq + term
    sine = -1.0 / 39916800.0
    for term in (1.0 / 362880.0, -1.0 / 5040.0, 1.0 / 120.0, -1.0 / 6.0, 1.0):
        sine = sine * sq + term
    return cosine * sign, sine * angle * sign


def grid_kernel(pts_ref, inv_ref, wave_ref, coef_ref, weights_ref, out_ref, table, tend, *, items):
    waves = wave_ref.shape[0]
    points = coef_ref.shape[1]
    rows = weights_ref.shape[2]
    wave = wave_ref[...]
    lane = lax.broadcasted_iota(jnp.int32, (1, LANES), 1)
    lane_f = lane.astype(jnp.float32)

    def one(pos, slot):
        pts = pts_ref[pos]
        pts_f = pts.astype(jnp.float32)
        inv = inv_ref[pos]
        prod = wave * lane_f
        left = prod - jnp.floor(prod * inv) * pts_f
        cosine, sine = unit_circle(left * inv)
        live = jnp.where(2.0 * wave < pts_f, 1.0, 0.0)
        mid_c = cosine[:, LANES // 2:LANES // 2 + 1]
        mid_s = sine[:, LANES // 2:LANES // 2 + 1]
        step_c = jnp.broadcast_to(1.0 - 2.0 * mid_s * mid_s, (waves, LANES))
        step_s = jnp.broadcast_to(2.0 * mid_s * mid_c, (waves, LANES))
        cosine = cosine * live
        sine = -sine * live
        for hi in range(points // LANES):
            inside = hi * LANES + lane < pts
            cols = slice(hi * LANES, (hi + 1) * LANES)
            table[slot, 0:waves, cols] = jnp.where(inside, cosine, 0.0).astype(jnp.bfloat16)
            table[slot, waves:2 * waves, cols] = jnp.where(inside, sine, 0.0).astype(jnp.bfloat16)
            cosine, sine = (
                cosine * step_c + sine * step_s,
                sine * step_c - cosine * step_s,
            )
        weights = weights_ref[pos]
        for start in range(0, points, CHUNK):
            cols = slice(start, start + CHUNK)
            grid = lax.dot_general(
                weights, table[slot, :, cols], (((0,), (0,)), ((), ())),
                preferred_element_type=jnp.float32,
            )
            coef = coef_ref[pl.ds(pos, 1), cols]
            for first in range(0, rows, 3 * items):
                parts = [grid[first + f * items:first + (f + 1) * items] for f in range(3)]
                for f in range(3):
                    value = parts[f] * (coef + parts[(f + 1) % 3])
                    low = first + f * items
                    tend[slot, low:low + items, cols] = value.astype(jnp.bfloat16)
        back = lax.dot_general(
            table[slot], tend[slot], (((1,), (1,)), ((), ())),
            preferred_element_type=jnp.float32,
        )
        out_ref[pos] = (back * inv).astype(jnp.bfloat16)

    count = coef_ref.shape[0]
    together = UNROLL if count % UNROLL == 0 else 1

    def step(index, carry):
        for slot in range(together):
            one(index * together + slot, slot)
        return carry

    lax.fori_loop(0, count // together, step, 0)


def grid_trip(weights, wave_ids, counts, coefs, items):
    count, modes, rows = weights.shape
    waves = wave_ids.shape[0]
    points = coefs.shape[1]
    wave_f = jnp.broadcast_to(wave_ids.astype(jnp.float32)[:, None], (waves, LANES))
    smem = pl.BlockSpec(memory_space=pltpu.SMEM)
    vmem = pl.BlockSpec(memory_space=pltpu.VMEM)
    return pl.pallas_call(
        functools.partial(grid_kernel, items=items),
        in_specs=[smem, smem, vmem, vmem, vmem],
        out_specs=vmem,
        out_shape=jax.ShapeDtypeStruct((count, modes, rows), jnp.bfloat16),
        scratch_shapes=[
            pltpu.VMEM((UNROLL, modes, points), jnp.bfloat16),
            pltpu.VMEM((UNROLL, rows, points), jnp.bfloat16),
        ],
    )(counts, 1.0 / counts.astype(jnp.float32), wave_f, coefs, weights)


def on_device(
    spectral,
    legendre,
    wave_ids,
    trunc_lengths,
    cycle_points,
    grid_coef,
    cycle_weights,
    modes_in,
    modes_out,
    depths,
):
    wave_size = lax.axis_size("wave")
    lev_size = lax.axis_size("lev")
    wave_rank = lax.axis_index("wave")
    lev_rank = lax.axis_index("lev")
    wave_local, channels, lev_local, spec_len = spectral.shape
    half_lat = legendre.shape[1]
    wave_total = wave_ids.shape[0]
    fields = channels // 2
    levels = lev_local * lev_size
    items = channels * lev_local
    everyone = wave_size * lev_size
    band = 2 * half_lat // wave_size
    sub = band // lev_size
    north_bands = wave_size // 2
    own_waves = lax.dynamic_slice_in_dim(wave_ids, wave_rank * wave_local, wave_local)
    own_lengths = lax.dynamic_slice_in_dim(trunc_lengths, wave_rank * wave_local, wave_local)
    position = jnp.arange(spec_len, dtype=jnp.int32)

    flip = wave_rank >= north_bands
    north_rank = jnp.where(flip, wave_size - 1 - wave_rank, wave_rank)
    counts = lax.dynamic_slice_in_dim(cycle_points, north_rank * band + lev_rank * sub, sub)
    coef_row = jnp.where(flip, band - (lev_rank + 1) * sub, lev_rank * sub)
    coefs = lax.dynamic_slice_in_dim(grid_coef, coef_row, sub, 0)
    coefs = jnp.where(flip, coefs[::-1], coefs)

    factor = jnp.where(own_waves == 0, 1.0, 2.0).astype(jnp.bfloat16)
    live = (position[None, :] < own_lengths[:, None])[:, None, :]
    flat = spectral.reshape(wave_local, items, spec_len) * factor[:, None, None]
    zero = jnp.zeros_like(flat)
    even_in = jnp.where(live & (position % 2 == 0), flat, zero)
    odd_in = jnp.where(live & (position % 2 == 1), flat, zero)
    both = jnp.concatenate([even_in, odd_in], axis=1)
    sums = jnp.einsum("mji,mri->mjr", legendre, both, preferred_element_type=jnp.float32)
    even_sum, odd_sum = sums[..., :items], sums[..., items:]
    north = (even_sum + odd_sum).astype(jnp.bfloat16)
    south = (even_sum - odd_sum).astype(jnp.bfloat16)

    def banded(part):
        rows = jnp.swapaxes(part, 0, 1)
        return rows.reshape(north_bands, lev_size, sub, wave_local * items)

    blocks = jnp.concatenate([banded(north), banded(south)[::-1]], axis=0)
    blocks = blocks.reshape(everyone, sub, wave_local * items)

    share = wave_local * channels // lev_size
    parts_of_r = share // fields
    first = sub // 16 * 8
    cuts = [(0, first), (first, sub)] if sub % 8 == 0 and first else [(0, sub)]
    pieces = []
    for low, high in cuts:
        size = high - low
        got = lax.all_to_all(
            blocks[:, low:high], ("wave", "lev"), split_axis=0, concat_axis=0, tiled=True
        )
        weights = got.reshape(wave_size, lev_size, size, wave_local, 2, fields * lev_local)
        weights = weights.transpose(2, 4, 0, 3, 1, 5)
        weights = weights.reshape(size, 2 * wave_total, fields * levels)
        analysed = grid_trip(weights, wave_ids, counts[low:high], coefs[low:high], lev_local)
        sent = analysed.reshape(size, 2 // parts_of_r, parts_of_r, wave_total, fields * levels)
        sent = sent.transpose(3, 1, 0, 2, 4).reshape(everyone, size, share * levels)
        pieces.append(
            lax.all_to_all(sent, ("wave", "lev"), split_axis=0, concat_axis=0, tiled=True)
        )
    back = jnp.concatenate(pieces, axis=1) if len(pieces) > 1 else pieces[0]
    back = back.reshape(2, north_bands, band, share * levels)
    northern = back[0].reshape(half_lat, share * levels).astype(jnp.float32)
    southern = back[1][::-1].reshape(half_lat, share * levels).astype(jnp.float32)
    scale = cycle_weights[:, None]
    even = (scale * (northern + southern)).astype(jnp.bfloat16)
    odd = (scale * (northern - southern)).astype(jnp.bfloat16)
    per_wave = channels // share
    column = lev_rank // per_wave
    own_polys = lax.dynamic_index_in_dim(legendre, column, 0, keepdims=False)
    own_wave = lax.dynamic_index_in_dim(own_waves, column, 0, keepdims=False)
    own_length = lax.dynamic_index_in_dim(own_lengths, column, 0, keepdims=False)
    from_even = jnp.einsum("jr,ji->ri", even, own_polys, preferred_element_type=jnp.float32)
    from_odd = jnp.einsum("jr,ji->ri", odd, own_polys, preferred_element_type=jnp.float32)
    projected = jnp.where(position % 2 == 0, from_even, from_odd)
    projected = jnp.where(position < own_length, projected, 0.0).astype(jnp.bfloat16)
    projected = projected.reshape(parts_of_r, lev_size, fields, lev_local, spec_len)
    projected = projected.transpose(0, 2, 1, 3, 4).reshape(share, levels, spec_len)
    mode_vals = jnp.einsum("ql,cli->cqi", modes_in, projected, preferred_element_type=jnp.float32)
    degree = (own_wave + position).astype(jnp.float32)
    damp = 1.0 / (1.0 + depths[:, None] * degree * (degree + 1.0) / float(spec_len * spec_len))
    scaled = (mode_vals * damp).astype(jnp.bfloat16)
    update = jnp.einsum(
        "lq,cqi->cli", modes_out, scaled, preferred_element_type=jnp.float32
    ).astype(jnp.bfloat16)
    update = lax.all_to_all(update, "lev", split_axis=1, concat_axis=0, tiled=True)
    return update.reshape(wave_local, channels, lev_local, spec_len)


def solution(mesh):
    placed = (
        P("wave", None, "lev", None),
        P("wave", None, None),
        P(),
        P(),
        P(),
        P("wave", None),
        P(),
        P(),
        P(),
        P(),
    )
    return jax.shard_map(
        on_device,
        mesh=mesh,
        in_specs=placed,
        out_specs=P("wave", None, "lev", None),
        check_vma=False,
    )
```

```python
import functools

import jax
import jax.numpy as jnp
from jax import lax
from jax.experimental import pallas as pl
from jax.experimental.pallas import tpu as pltpu
from jax.sharding import PartitionSpec as P

LANES = 128
UNROLL = 8
CHUNK = 512


def unit_circle(turns):
    half = jnp.floor(2.0 * turns + 0.5)
    angle = (turns - 0.5 * half) * (2.0 * jnp.pi)
    sign = jnp.where(half == 1.0, -1.0, 1.0)
    sq = angle * angle
    cosine = -1.0 / 3628800.0
    for term in (1.0 / 40320.0, -1.0 / 720.0, 1.0 / 24.0, -0.5, 1.0):
        cosine = cosine * sq + term
    sine = -1.0 / 39916800.0
    for term in (1.0 / 362880.0, -1.0 / 5040.0, 1.0 / 120.0, -1.0 / 6.0, 1.0):
        sine = sine * sq + term
    return cosine * sign, sine * angle * sign


def grid_kernel(
    pts_ref, inv_ref, flip_ref, wave_ref, coef_ref, weights_ref, out_ref, table, tend, *, items, first
):
    waves = wave_ref.shape[0]
    points = coef_ref.shape[1]
    rows = weights_ref.shape[2]
    wave = wave_ref[...]
    lane = lax.broadcasted_iota(jnp.int32, (1, LANES), 1)
    lane_f = lane.astype(jnp.float32)

    def one(pos, slot):
        pts = pts_ref[first + pos]
        pts_f = pts.astype(jnp.float32)
        inv = inv_ref[first + pos]
        prod = wave * lane_f
        left = prod - jnp.floor(prod * inv) * pts_f
        cosine, sine = unit_circle(left * inv)
        live = jnp.where(2.0 * wave < pts_f, 1.0, 0.0)
        mid_c = cosine[:, LANES // 2:LANES // 2 + 1]
        mid_s = sine[:, LANES // 2:LANES // 2 + 1]
        step_c = jnp.broadcast_to(1.0 - 2.0 * mid_s * mid_s, (waves, LANES))
        step_s = jnp.broadcast_to(2.0 * mid_s * mid_c, (waves, LANES))
        cosine = cosine * live
        sine = -sine * live
        for hi in range(points // LANES):
            inside = hi * LANES + lane < pts
            cols = slice(hi * LANES, (hi + 1) * LANES)
            table[slot, 0:waves, cols] = jnp.where(inside, cosine, 0.0).astype(jnp.bfloat16)
            table[slot, waves:2 * waves, cols] = jnp.where(inside, sine, 0.0).astype(jnp.bfloat16)
            cosine, sine = (
                cosine * step_c + sine * step_s,
                sine * step_c - cosine * step_s,
            )
        weights = weights_ref[pos]
        row = jnp.where(flip_ref[0] == 1, coef_ref.shape[0] - 1 - first - pos, first + pos)
        for start in range(0, points, CHUNK):
            cols = slice(start, start + CHUNK)
            grid = lax.dot_general(
                weights, table[slot, :, cols], (((0,), (0,)), ((), ())),
                preferred_element_type=jnp.float32,
            )
            coef = coef_ref[pl.ds(row, 1), cols]
            for base in range(0, rows, 3 * items):
                parts = [grid[base + f * items:base + (f + 1) * items] for f in range(3)]
                for f in range(3):
                    value = parts[f] * (coef + parts[(f + 1) % 3])
                    low = base + f * items
                    tend[slot, low:low + items, cols] = value.astype(jnp.bfloat16)
        back = lax.dot_general(
            table[slot], tend[slot], (((1,), (1,)), ((), ())),
            preferred_element_type=jnp.float32,
        )
        out_ref[pos] = (back * inv).astype(jnp.bfloat16)

    count = weights_ref.shape[0]
    together = UNROLL if count % UNROLL == 0 else 1

    def step(index, carry):
        for slot in range(together):
            one(index * together + slot, slot)
        return carry

    lax.fori_loop(0, count // together, step, 0)


def grid_trip(weights, wave_f, counts, inverse, flip, coefs, items, first):
    count, modes, rows = weights.shape
    points = coefs.shape[1]
    smem = pl.BlockSpec(memory_space=pltpu.SMEM)
    vmem = pl.BlockSpec(memory_space=pltpu.VMEM)
    return pl.pallas_call(
        functools.partial(grid_kernel, items=items, first=first),
        in_specs=[smem, smem, smem, vmem, vmem, vmem],
        out_specs=vmem,
        out_shape=jax.ShapeDtypeStruct((count, modes, rows), jnp.bfloat16),
        scratch_shapes=[
            pltpu.VMEM((UNROLL, modes, points), jnp.bfloat16),
            pltpu.VMEM((UNROLL, rows, points), jnp.bfloat16),
        ],
    )(counts, inverse, flip, wave_f, coefs, weights)


def trade_levels(update, lev_size, lev_rank):
    share, levels, spec_len = update.shape
    lev_local = levels // lev_size

    def piece(rank):
        return lax.dynamic_slice_in_dim(update, rank * lev_local, lev_local, 1)

    joined = jnp.zeros((lev_size * share, lev_local, spec_len), update.dtype)
    joined = lax.dynamic_update_slice_in_dim(joined, piece(lev_rank), lev_rank * share, 0)
    arrived = []
    for mask in [*range(2, lev_size), 1]:
        pairs = [(rank, rank ^ mask) for rank in range(lev_size)]
        arrived.append((mask, lax.ppermute(piece(lev_rank ^ mask), "lev", pairs)))
    for mask, got in arrived:
        joined = lax.dynamic_update_slice_in_dim(joined, got, (lev_rank ^ mask) * share, 0)
    return joined


def on_device(
    spectral,
    legendre,
    wave_ids,
    trunc_lengths,
    cycle_points,
    grid_coef,
    cycle_weights,
    modes_in,
    modes_out,
    depths,
):
    wave_size = lax.axis_size("wave")
    lev_size = lax.axis_size("lev")
    wave_rank = lax.axis_index("wave")
    lev_rank = lax.axis_index("lev")
    wave_local, channels, lev_local, spec_len = spectral.shape
    half_lat = legendre.shape[1]
    wave_total = wave_ids.shape[0]
    fields = channels // 2
    levels = lev_local * lev_size
    items = channels * lev_local
    everyone = wave_size * lev_size
    band = 2 * half_lat // wave_size
    sub = band // lev_size
    north_bands = wave_size // 2
    own_waves = lax.dynamic_slice_in_dim(wave_ids, wave_rank * wave_local, wave_local)
    own_lengths = lax.dynamic_slice_in_dim(trunc_lengths, wave_rank * wave_local, wave_local)
    position = jnp.arange(spec_len, dtype=jnp.int32)

    flip = wave_rank >= north_bands
    north_rank = jnp.where(flip, wave_size - 1 - wave_rank, wave_rank)
    counts = lax.dynamic_slice_in_dim(cycle_points, north_rank * band + lev_rank * sub, sub)
    coef_row = jnp.where(flip, band - (lev_rank + 1) * sub, lev_rank * sub)
    coefs = lax.dynamic_slice_in_dim(grid_coef, coef_row, sub, 0)
    inverse = 1.0 / counts.astype(jnp.float32)
    flipped = flip.astype(jnp.int32)[None]
    wave_f = jnp.broadcast_to(wave_ids.astype(jnp.float32)[:, None], (wave_total, LANES))

    factor = jnp.where(own_waves == 0, 1.0, 2.0).astype(jnp.bfloat16)
    live = (position[None, :] < own_lengths[:, None])[:, None, :]
    flat = spectral.reshape(wave_local, items, spec_len) * factor[:, None, None]
    zero = jnp.zeros_like(flat)
    even_in = jnp.where(live & (position % 2 == 0), flat, zero)
    odd_in = jnp.where(live & (position % 2 == 1), flat, zero)
    both = jnp.concatenate([even_in, odd_in], axis=1)
    sums = jnp.einsum("mji,mri->mjr", legendre, both, preferred_element_type=jnp.float32)
    even_sum, odd_sum = sums[..., :items], sums[..., items:]
    north = (even_sum + odd_sum).astype(jnp.bfloat16)
    south = (even_sum - odd_sum).astype(jnp.bfloat16)

    def banded(part):
        rows = jnp.swapaxes(part, 0, 1)
        return rows.reshape(north_bands, lev_size, sub, wave_local * items)

    blocks = jnp.concatenate([banded(north), banded(south)[::-1]], axis=0)
    blocks = blocks.reshape(everyone, sub, wave_local * items)

    share = wave_local * channels // lev_size
    parts_of_r = share // fields
    first = sub // 16 * 8
    cuts = [(0, first), (first, sub)] if sub % 8 == 0 and first else [(0, sub)]
    pieces = []
    for low, high in cuts:
        size = high - low
        got = lax.all_to_all(
            blocks[:, low:high], ("wave", "lev"), split_axis=0, concat_axis=0, tiled=True
        )
        weights = got.reshape(wave_size, lev_size, size, wave_local, 2, fields * lev_local)
        weights = weights.transpose(2, 4, 0, 3, 1, 5)
        weights = weights.reshape(size, 2 * wave_total, fields * levels)
        analysed = grid_trip(weights, wave_f, counts, inverse, flipped, coefs, lev_local, low)
        sent = analysed.reshape(size, 2 // parts_of_r, parts_of_r, wave_total, fields * levels)
        sent = sent.transpose(3, 1, 0, 2, 4).reshape(everyone, size, share * levels)
        pieces.append(
            lax.all_to_all(sent, ("wave", "lev"), split_axis=0, concat_axis=0, tiled=True)
        )
    back = jnp.concatenate(pieces, axis=1) if len(pieces) > 1 else pieces[0]
    back = back.reshape(2, north_bands, band, share * levels)
    northern = back[0].reshape(half_lat, share * levels).astype(jnp.float32)
    southern = back[1][::-1].reshape(half_lat, share * levels).astype(jnp.float32)
    scale = cycle_weights[:, None]
    even = (scale * (northern + southern)).astype(jnp.bfloat16)
    odd = (scale * (northern - southern)).astype(jnp.bfloat16)
    per_wave = channels // share
    column = lev_rank // per_wave
    own_polys = lax.dynamic_index_in_dim(legendre, column, 0, keepdims=False)
    own_wave = lax.dynamic_index_in_dim(own_waves, column, 0, keepdims=False)
    own_length = lax.dynamic_index_in_dim(own_lengths, column, 0, keepdims=False)
    from_even = jnp.einsum("jr,ji->ri", even, own_polys, preferred_element_type=jnp.float32)
    from_odd = jnp.einsum("jr,ji->ri", odd, own_polys, preferred_element_type=jnp.float32)
    projected = jnp.where(position % 2 == 0, from_even, from_odd)
    projected = jnp.where(position < own_length, projected, 0.0).astype(jnp.bfloat16)
    projected = projected.reshape(parts_of_r, lev_size, fields, lev_local, spec_len)
    projected = projected.transpose(0, 2, 1, 3, 4).reshape(share, levels, spec_len)
    mode_vals = jnp.einsum("ql,cli->cqi", modes_in, projected, preferred_element_type=jnp.float32)
    degree = (own_wave + position).astype(jnp.float32)
    damp = 1.0 / (1.0 + depths[:, None] * degree * (degree + 1.0) / float(spec_len * spec_len))
    scaled = (mode_vals * damp).astype(jnp.bfloat16)
    update = jnp.einsum(
        "lq,cqi->cli", modes_out, scaled, preferred_element_type=jnp.float32
    ).astype(jnp.bfloat16)
    update = trade_levels(update, lev_size, lev_rank)
    return update.reshape(wave_local, channels, lev_local, spec_len)


def solution(mesh):
    placed = (
        P("wave", None, "lev", None),
        P("wave", None, None),
        P(),
        P(),
        P(),
        P("wave", None),
        P(),
        P(),
        P(),
        P(),
    )
    return jax.shard_map(
        on_device,
        mesh=mesh,
        in_specs=placed,
        out_specs=P("wave", None, "lev", None),
        check_vma=False,
    )
```
